8 devices in a mesh: dp: 2 (over y, z), sp: 4 (over x, core).
Axes of the slice: x: 2, y: 2, z: 1, core: 2. Of those that a mesh axis runs over, the one named last changes fastest.
Arguments:
- q: bfloat16 [64, 80, 80], P('dp'), parts along dimension 0
- k: bfloat16 [64, 8192, 8, 80], P('dp', 'sp'), parts along dimension 0
- v: bfloat16 [64, 8192, 8, 80], P('dp', 'sp'), parts along dimension 0
Outputs:
- q: bfloat16 [64, 80, 80], P('dp'), parts along dimension 0
There are 2 independent parts. The reference program is written for one: setup_inputs(seed, part) draws one part's arguments, and reference() takes and returns one part's arrays. A program takes and returns all parts, laid end to end along the dimension named above; each array names one.
All inputs are finite; a program needn't handle non-finite values.
Results may differ from the reference program's by a relative error of at most 0.012.
Values are sent between devices in bfloat16 or wider.
A program may use at most 2 GiB of HBM per device.

```python
import jax
import jax.numpy as jnp

BATCH = 32
CACHE = 8192
HEADS = 80
KV_HEADS = 8
HEAD = 80


def setup_inputs(seed: int = 0, part: int = 0) -> dict:
    kq, kk, kv = (jax.random.fold_in(k, part) for k in jax.random.split(jax.random.key(seed), 3))
    return {
        "q": (3 * jax.random.normal(kq, (BATCH, HEADS, HEAD), jnp.float32)).astype(jnp.bfloat16),
        "k": jax.random.normal(kk, (BATCH, CACHE, KV_HEADS, HEAD), jnp.float32).astype(jnp.bfloat16),
        "v": jax.random.normal(kv, (BATCH, CACHE, KV_HEADS, HEAD), jnp.float32).astype(jnp.bfloat16),
    }


def einsum(form, a, b):
    return jnp.einsum(form, a.astype(jnp.float32), b.astype(jnp.float32))


def reference(q, k, v):
    grouped = q.reshape(BATCH, KV_HEADS, -1, HEAD)
    scores = einsum("bgsd,bugd->bgsu", grouped, k) * HEAD**-0.5
    weights = jax.nn.softmax(scores, -1).astype(jnp.bfloat16)
    return einsum("bgsu,bugd->bgsd", weights, v).astype(jnp.bfloat16).reshape(BATCH, HEADS, HEAD)
```

```python
import math

import jax
import jax.numpy as jnp
from jax import lax
from jax.experimental import pallas as pl
from jax.experimental.pallas import tpu as pltpu
from jax.sharding import PartitionSpec as P

DEPTH = 4
LAG = 3
F32, BF16 = jnp.float32, jnp.bfloat16


def kernel(n, groups, share, q_ref, k_hbm, v_hbm, out_ref, kbuf, vbuf, spread, pick, qbd, prob, parts, stats, ksem, vsem, send_sem, recv_sem):
    count, heads, head = q_ref.shape
    rows, run = kbuf.shape[1], kbuf.shape[2]
    factor = head**-0.5 * math.log2(math.e)
    me = lax.axis_index("sp")
    peers = [lax.rem(me + d, n) for d in range(1, n)]

    def fetch(i, hbm, buf, sem):
        slot = lax.rem(i, DEPTH)
        return pltpu.make_async_copy(hbm.at[i], buf.at[slot], sem.at[slot])

    def sends(i):
        return [
            pltpu.make_async_remote_copy(
                src_ref=ref.at[me, i],
                dst_ref=ref.at[me, i],
                send_sem=send_sem.at[i, 2 * d + r],
                recv_sem=recv_sem.at[i, 2 * d + r],
                device_id={"sp": peer},
                device_id_type=pl.DeviceIdType.MESH,
            )
            for d, peer in enumerate(peers)
            for r, ref in enumerate((parts, stats))
        ]

    barrier = pltpu.get_barrier_semaphore()
    for peer in peers:
        pl.semaphore_signal(barrier, inc=1, device_id={"sp": peer}, device_id_type=pl.DeviceIdType.MESH)

    for i in range(DEPTH):
        fetch(i, k_hbm, kbuf, ksem).start()
        fetch(i, v_hbm, vbuf, vsem).start()

    lane = lax.broadcasted_iota(jnp.int32, (head, rows), 1)
    row = lax.broadcasted_iota(jnp.int32, (head, rows), 0)
    spread[...] = (lax.rem(lane, head) == row).astype(F32).astype(BF16)
    lane = lax.broadcasted_iota(jnp.int32, (heads, rows), 1)
    row = lax.broadcasted_iota(jnp.int32, (heads, rows), 0)
    pick[...] = (lane // head == row // share).astype(F32).astype(BF16)
    column = lax.broadcasted_iota(jnp.int32, (head, heads), 1)

    def widen(i):
        wide = jnp.dot(q_ref[i], spread[...], preferred_element_type=F32).astype(BF16)
        qbd[lax.rem(i, 2)] = wide * pick[...]

    def weigh(i):
        s = jnp.dot(qbd[lax.rem(i, 2)], kbuf[lax.rem(i, DEPTH)], preferred_element_type=F32)
        high = jnp.max(s, -1, keepdims=True)
        p = jnp.exp2((s - high) * factor)
        total = jnp.sum(p, -1, keepdims=True)
        prob[lax.rem(i, 2)] = p.astype(BF16)
        spot = lax.broadcasted_iota(jnp.int32, (heads, 128), 1)
        both = jnp.where(spot == 0, high, total)
        stats[me, i, :, :heads] = both.T[:8]

    def add_up(i):
        slot, w = lax.rem(i, DEPTH), prob[lax.rem(i, 2)]
        half = rows // 2
        part = jnp.zeros((head, heads), F32)
        for a in range(2):
            seen = lax.dot_general(
                vbuf[slot, a * half : (a + 1) * half], w, (((1,), (1,)), ((), ())), preferred_element_type=F32
            )
            for b in range(groups // 2):
                g = a * groups // 2 + b
                here = (column >= g * share) & (column < (g + 1) * share)
                part = jnp.where(here, seen[b * head : (b + 1) * head], part)
        parts[me, i] = part.astype(BF16)

    def together(i):
        for copy in sends(i):
            copy.wait_recv()
        high = [stats[d, i, 0:1, :heads] for d in range(n)]
        total = [stats[d, i, 1:2, :heads] for d in range(n)]
        top = high[0]
        for h in high[1:]:
            top = jnp.maximum(top, h)
        scale = [jnp.exp2((h - top) * factor) for h in high]
        whole = total[0] * scale[0]
        for t, c in zip(total[1:], scale[1:]):
            whole += t * c
        acc = parts[0, i].astype(F32) * scale[0]
        for d in range(1, n):
            acc += parts[d, i].astype(F32) * scale[d]
        out_ref[i] = (acc / whole).T.astype(BF16)

    widen(0)
    widen(1)
    fetch(0, k_hbm, kbuf, ksem).wait()
    weigh(0)
    pl.semaphore_wait(barrier, n - 1)

    def step(i, carry):
        @pl.when(i - 1 + DEPTH < count)
        def _():
            fetch(i - 1 + DEPTH, k_hbm, kbuf, ksem).start()

        @pl.when((i >= 2) & (i - 2 + DEPTH < count))
        def _():
            fetch(i - 2 + DEPTH, v_hbm, vbuf, vsem).start()

        @pl.when(i >= 2)
        def _():
            for copy in sends(i - 2):
                copy.start()

        @pl.when(i >= 1 + LAG)
        def _():
            together(i - 1 - LAG)

        fetch(i, k_hbm, kbuf, ksem).wait()
        fetch(i - 1, v_hbm, vbuf, vsem).wait()
        weigh(i)
        add_up(i - 1)
        widen(jnp.minimum(i + 1, count - 1))
        return carry

    lax.fori_loop(1, count, step, 0)

    for copy in sends(count - 2):
        copy.start()
    fetch(count - 1, v_hbm, vbuf, vsem).wait()
    add_up(count - 1)
    for copy in sends(count - 1):
        copy.start()

    def rest(i, carry):
        together(i)
        return carry

    lax.fori_loop(count - 1 - LAG, count, rest, 0)

    def drain(i, carry):
        for copy in sends(i):
            copy.wait_send()
        return carry

    lax.fori_loop(0, count, drain, 0)


def solution(mesh):
    n = mesh.shape["sp"]

    def step(q, k, v):
        count, run, groups, head = k.shape
        heads = q.shape[1]
        rows = groups * head
        k, v = (a.transpose(0, 2, 3, 1).reshape(count, rows, run) for a in (k, v))

        def body(*refs):
            kernel(n, groups, heads // groups, *refs)

        return pl.pallas_call(
            body,
            out_shape=jax.ShapeDtypeStruct((count, heads, head), BF16),
            in_specs=[
                pl.BlockSpec(memory_space=pltpu.VMEM),
                pl.BlockSpec(memory_space=pl.ANY),
                pl.BlockSpec(memory_space=pl.ANY),
            ],
            out_specs=pl.BlockSpec(memory_space=pltpu.VMEM),
            scratch_shapes=[
                pltpu.VMEM((DEPTH, rows, run), BF16),
                pltpu.VMEM((DEPTH, rows, run), BF16),
                pltpu.VMEM((head, rows), BF16),
                pltpu.VMEM((heads, rows), BF16),
                pltpu.VMEM((2, heads, rows), BF16),
                pltpu.VMEM((2, heads, run), BF16),
                pltpu.VMEM((n, count, head, heads), BF16),
                pltpu.VMEM((n, count, 8, 128), F32),
                pltpu.SemaphoreType.DMA((DEPTH,)),
                pltpu.SemaphoreType.DMA((DEPTH,)),
                pltpu.SemaphoreType.DMA((count, 2 * (n - 1))),
                pltpu.SemaphoreType.DMA((count, 2 * (n - 1))),
            ],
            compiler_params=pltpu.CompilerParams(
                collective_id=0, has_side_effects=True, vmem_limit_bytes=60000 * 1024
            ),
        )(q, k, v)

    return jax.shard_map(
        step,
        mesh=mesh,
        in_specs=(P("dp", None, None), P("dp", "sp", None, None), P("dp", "sp", None, None)),
        out_specs=P("dp", None, None),
        check_vma=False,
    )
```

```python
import math

import jax
import jax.numpy as jnp
from jax import lax
from jax.experimental import pallas as pl
from jax.experimental.pallas import tpu as pltpu
from jax.sharding import PartitionSpec as P

DEPTH = 4
LAG = 4
RING = 2 * LAG + 1
PAD = 256
F32, BF16 = jnp.float32, jnp.bfloat16
MESH = pl.DeviceIdType.MESH


def kernel(n, groups, share, q_hbm, k_hbm, v_hbm, out_ref, q_ref, kbuf, vbuf, spread, pick, qbd0, qbd1, prob0, prob1, parts, stats, qsem, ksem, vsem, send_sem, recv_sem):
    count, heads, head = q_ref.shape
    rows, run = k_hbm.shape[1], k_hbm.shape[2]
    factor = head**-0.5 * math.log2(math.e)
    me = lax.axis_index("sp")
    peers = [lax.rem(me + d, n) for d in range(1, n)]
    qbd, prob = (qbd0, qbd1), (prob0, prob1)

    def fetch(i, hbm, buf, sem):
        slot = lax.rem(i, DEPTH)
        return pltpu.make_async_copy(hbm.at[i], buf.at[slot, :, :run], sem.at[slot])

    def sends(i):
        slot = lax.rem(i, RING)
        return [
            pltpu.make_async_remote_copy(
                src_ref=ref.at[me, slot],
                dst_ref=ref.at[me, slot],
                send_sem=send_sem.at[slot, 2 * d + r],
                recv_sem=recv_sem.at[slot, 2 * d + r],
                device_id={"sp": peer},
                device_id_type=MESH,
            )
            for d, peer in enumerate(peers)
            for r, ref in enumerate((parts, stats))
        ]

    for i in range(DEPTH):
        fetch(i, k_hbm, kbuf, ksem).start()
        if i == 0:
            pltpu.make_async_copy(q_hbm, q_ref, qsem).start()
        fetch(i, v_hbm, vbuf, vsem).start()

    barrier = pltpu.get_barrier_semaphore()
    for peer in peers:
        pl.semaphore_signal(barrier, inc=1, device_id={"sp": peer}, device_id_type=MESH)

    lane = lax.broadcasted_iota(jnp.int32, (head, rows), 1)
    row = lax.broadcasted_iota(jnp.int32, (head, rows), 0)
    spread[...] = (lax.rem(lane, head) == row).astype(F32).astype(BF16)
    lane = lax.broadcasted_iota(jnp.int32, (heads, rows), 1)
    row = lax.broadcasted_iota(jnp.int32, (heads, rows), 0)
    pick[...] = (lane // head == row // share).astype(F32).astype(BF16)
    column = lax.broadcasted_iota(jnp.int32, (head, heads), 1)

    def widen(i, side):
        wide = jnp.dot(q_ref[i], spread[...], preferred_element_type=F32).astype(BF16)
        qbd[side][...] = wide * pick[...]

    def weigh(i, side):
        s = jnp.dot(qbd[side][...], kbuf[lax.rem(i, DEPTH), :, :run], preferred_element_type=F32)
        high = jnp.max(s, -1, keepdims=True)
        p = jnp.exp2((s - high) * factor)
        total = jnp.sum(p, -1, keepdims=True)
        prob[side][...] = p.astype(BF16)
        spot = lax.broadcasted_iota(jnp.int32, (heads, 128), 1)
        both = jnp.where(spot == 0, high, total)
        stats[me, lax.rem(i, RING), :, :heads] = both.T[:8]

    def add_up(i, side):
        slot, w = lax.rem(i, DEPTH), prob[side][...]
        half = rows // 2
        part = jnp.zeros((head, heads), F32)
        for a in range(2):
            seen = lax.dot_general(
                vbuf[slot, a * half : (a + 1) * half, :run], w, (((1,), (1,)), ((), ())), preferred_element_type=F32
            )
            for b in range(groups // 2):
                g = a * groups // 2 + b
                here = (column >= g * share) & (column < (g + 1) * share)
                part = jnp.where(here, seen[b * head : (b + 1) * head], part)
        parts[me, lax.rem(i, RING)] = part.astype(BF16)

    def arrive(i):
        for copy in sends(i):
            copy.wait_send()
            copy.wait_recv()

    def together(i):
        slot = lax.rem(i, RING)
        high = [stats[d, slot, 0:1, :heads] for d in range(n)]
        total = [stats[d, slot, 1:2, :heads] for d in range(n)]
        top = high[0]
        for h in high[1:]:
            top = jnp.maximum(top, h)
        scale = [jnp.exp2((h - top) * factor) for h in high]
        whole = total[0] * scale[0]
        for t, c in zip(total[1:], scale[1:]):
            whole += t * c
        acc = parts[0, slot].astype(F32) * scale[0]
        for d in range(1, n):
            acc += parts[d, slot].astype(F32) * scale[d]
        out_ref[i] = (acc / whole).T.astype(BF16)

    def step(i, side, late):
        @pl.when(i - 1 + DEPTH < count)
        def _():
            fetch(i - 1 + DEPTH, k_hbm, kbuf, ksem).start()

        @pl.when((i >= 2) & (i - 2 + DEPTH < count))
        def _():
            fetch(i - 2 + DEPTH, v_hbm, vbuf, vsem).start()

        @pl.when(i >= 2)
        def _():
            for copy in sends(i - 2):
                copy.start()

        if late:
            arrive(i - 1 - LAG)
        fetch(i, k_hbm, kbuf, ksem).wait()
        fetch(i - 1, v_hbm, vbuf, vsem).wait()
        weigh(i, side)
        add_up(i - 1, 1 - side)
        widen(jnp.minimum(i + 1, count - 1), 1 - side)
        if late:
            together(i - 1 - LAG)

    pltpu.make_async_copy(q_hbm, q_ref, qsem).wait()
    widen(0, 0)
    widen(1, 1)
    fetch(0, k_hbm, kbuf, ksem).wait()
    weigh(0, 0)
    pl.semaphore_wait(barrier, n - 1)

    def pair(late, j, carry):
        step(2 * j + 1, 1, late)
        step(2 * j + 2, 0, late)
        return carry

    lax.fori_loop(0, LAG // 2, lambda j, c: pair(False, j, c), 0)
    lax.fori_loop(LAG // 2, count // 2 - 1, lambda j, c: pair(True, j, c), 0)
    step(count - 1, 1, True)

    for copy in sends(count - 2):
        copy.start()
    fetch(count - 1, v_hbm, vbuf, vsem).wait()
    add_up(count - 1, 1)
    for copy in sends(count - 1):
        copy.start()

    def rest(i, carry):
        arrive(i)
        together(i)
        return carry

    lax.fori_loop(count - 1 - LAG, count, rest, 0)


def solution(mesh):
    n = mesh.shape["sp"]

    def step(q, k, v):
        count, run, groups, head = k.shape
        heads = q.shape[1]
        rows = groups * head
        k, v = (a.transpose(0, 2, 3, 1).reshape(count, rows, run) for a in (k, v))

        def body(*refs):
            kernel(n, groups, heads // groups, *refs)

        return pl.pallas_call(
            body,
            out_shape=jax.ShapeDtypeStruct((count, heads, head), BF16),
            in_specs=[pl.BlockSpec(memory_space=pl.ANY)] * 3,
            out_specs=pl.BlockSpec(memory_space=pltpu.VMEM),
            scratch_shapes=[
                pltpu.VMEM((count, heads, head), BF16),
                pltpu.VMEM((DEPTH, rows, run + PAD), BF16),
                pltpu.VMEM((DEPTH, rows, run + PAD), BF16),
                pltpu.VMEM((head, rows), BF16),
                pltpu.VMEM((heads, rows), BF16),
                pltpu.VMEM((heads, rows), BF16),
                pltpu.VMEM((heads, rows), BF16),
                pltpu.VMEM((heads, run), BF16),
                pltpu.VMEM((heads, run), BF16),
                pltpu.VMEM((n, RING, head, heads), BF16),
                pltpu.VMEM((n, RING, 8, 128), F32),
                pltpu.SemaphoreType.DMA,
                pltpu.SemaphoreType.DMA((DEPTH,)),
                pltpu.SemaphoreType.DMA((DEPTH,)),
                pltpu.SemaphoreType.DMA((RING, 2 * (n - 1))),
                pltpu.SemaphoreType.DMA((RING, 2 * (n - 1))),
            ],
            compiler_params=pltpu.CompilerParams(
                collective_id=0, has_side_effects=True, vmem_limit_bytes=60000 * 1024
            ),
        )(q, k, v)

    return jax.shard_map(
        step,
        mesh=mesh,
        in_specs=(P("dp", None, None), P("dp", "sp", None, None), P("dp", "sp", None, None)),
        out_specs=P("dp", None, None),
        check_vma=False,
    )
```

```python
import math

import jax
import jax.numpy as jnp
from jax import lax
from jax.experimental import pallas as pl
from jax.experimental.pallas import tpu as pltpu
from jax.sharding import PartitionSpec as P

KDEPTH, VDEPTH = 4, 4
WAIT = 3
RING = 10
PAD = 256
TILE = 256
F32, BF16 = jnp.float32, jnp.bfloat16
MESH = pl.DeviceIdType.MESH


def kernel(n, groups, share, q_hbm, k_hbm, v_hbm, out_ref, q_ref, kbuf, vbuf, spread, pick, qbd0, qbd1, s0, s1, p0, p1, parts, stats, tally, qsem, ksem, vsem, send_sem, recv_sem):
    count, heads, head = q_ref.shape
    rows, run = k_hbm.shape[1], k_hbm.shape[2]
    half = rows // 2
    factor = head**-0.5 * math.log2(math.e)
    me = lax.axis_index("sp")
    peers = [lax.rem(me + d, n) for d in range(1, n)]
    qbd, score, prob = (qbd0, qbd1), (s0, s1), (p0, p1)

    def keys(i):
        slot = lax.rem(i, KDEPTH)
        return pltpu.make_async_copy(k_hbm.at[i], kbuf.at[slot, :, :run], ksem.at[slot])

    def values(i):
        slot = lax.rem(i, VDEPTH)
        return pltpu.make_async_copy(v_hbm.at[i], vbuf.at[slot, :, :run], vsem.at[slot])

    def sends(i):
        slot = lax.rem(i, RING)
        return [
            pltpu.make_async_remote_copy(
                src_ref=ref.at[me, slot],
                dst_ref=ref.at[me, slot],
                send_sem=send_sem.at[slot],
                recv_sem=recv_sem.at[slot],
                device_id={"sp": peer},
                device_id_type=MESH,
            )
            for peer in peers
            for ref in (parts, stats)
        ]

    def arrive(i):
        for sem in (send_sem, recv_sem):
            pltpu.make_async_copy(tally, tally, sem.at[lax.rem(i, RING)]).wait()

    def widen(i, side):
        wide = jnp.dot(q_ref[i], spread[...], preferred_element_type=F32).astype(BF16)
        qbd[side][...] = wide * pick[...]

    def together(i):
        slot = lax.rem(i, RING)
        high = [stats[d, slot, 0:1, :heads] for d in range(n)]
        total = [stats[d, slot, 1:2, :heads] for d in range(n)]
        top = high[0]
        for h in high[1:]:
            top = jnp.maximum(top, h)
        scale = [jnp.exp2((h - top) * factor) for h in high]
        whole = total[0] * scale[0]
        for t, c in zip(total[1:], scale[1:]):
            whole += t * c
        acc = parts[0, slot, :, :heads].astype(F32) * scale[0]
        for d in range(1, n):
            acc += parts[d, slot, :, :heads].astype(F32) * scale[d]
        out_ref[i] = (acc / whole).T.astype(BF16)

    def block(scores=None, soften=None, add=None):
        if soften is not None:
            s_in, p_out = soften[1:]
            high = s_in[:, :128]
            for c in range(128, run, 128):
                high = jnp.maximum(high, s_in[:, c : c + 128])
            high = jnp.max(high, -1, keepdims=True)
            total = jnp.zeros((heads, 128), F32)
        seen = {}
        for t in range(0, run, TILE):
            tile = slice(t, t + TILE)
            if add is not None:
                for a in range(2):
                    v = vbuf[lax.rem(add[0], VDEPTH), a * half : (a + 1) * half, tile]
                    d = lax.dot_general(v, add[1][:, tile], (((1,), (1,)), ((), ())), preferred_element_type=F32)
                    seen[a] = seen[a] + d if a in seen else d
            if scores is not None:
                i, q_in, s_out = scores
                s_out[:, tile] = jnp.dot(q_in[...], kbuf[lax.rem(i, KDEPTH), :, tile], preferred_element_type=F32)
            if soften is not None:
                p = jnp.exp2((s_in[:, tile] - high) * factor)
                p_out[:, tile] = p.astype(BF16)
                for c in range(0, TILE, 128):
                    total += p[:, c : c + 128]
        if soften is not None:
            total = jnp.sum(total, -1, keepdims=True)
            spot = lax.broadcasted_iota(jnp.int32, (heads, 128), 1)
            both = jnp.where(spot == 0, high, total)
            stats[me, lax.rem(soften[0], RING), :, :heads] = both.T[:2]
        if add is not None:
            column = lax.broadcasted_iota(jnp.int32, (head, heads), 1)
            part = jnp.zeros((head, heads), F32)
            for a in range(2):
                for b in range(groups // 2):
                    g = a * groups // 2 + b
                    here = (column >= g * share) & (column < (g + 1) * share)
                    part = jnp.where(here, seen[a][b * head : (b + 1) * head], part)
            parts[me, lax.rem(add[0], RING), :, :heads] = part.astype(BF16)

    def start(i):
        @pl.when(i - 1 + KDEPTH < count)
        def _():
            keys(i - 1 + KDEPTH).start()

        @pl.when(i - 3 + VDEPTH < count)
        def _():
            values(i - 3 + VDEPTH).start()

    def step(i, a, late, first=False):
        if first:

            @pl.when(i >= 3)
            def _():
                start(i)
                for copy in sends(i - 3):
                    copy.start()

            @pl.when(i < 3)
            def _():
                keys(i - 1 + KDEPTH).start()
        else:
            start(i)
            for copy in sends(i - 3):
                copy.start()
        if late:
            arrive(i - 3 - WAIT)
        keys(i).wait()
        values(i - 2).wait()
        if late:
            together(i - 3 - WAIT)
        widen(jnp.minimum(i + 1, count - 1), 1 - a)
        block((i, qbd[a], score[a]), (i - 1, score[1 - a], prob[1 - a]), (i - 2, prob[a]))

    keys(0).start()
    pltpu.make_async_copy(q_hbm, q_ref, qsem).start()
    for i in range(1, VDEPTH + 2):
        if i < KDEPTH:
            keys(i).start()
        if i >= 2:
            values(i - 2).start()

    barrier = pltpu.get_barrier_semaphore()
    for peer in peers:
        pl.semaphore_signal(barrier, inc=1, device_id={"sp": peer}, device_id_type=MESH)

    lane = lax.broadcasted_iota(jnp.int32, (head, rows), 1)
    row = lax.broadcasted_iota(jnp.int32, (head, rows), 0)
    spread[...] = (lax.rem(lane, head) == row).astype(F32).astype(BF16)
    lane = lax.broadcasted_iota(jnp.int32, (heads, rows), 1)
    row = lax.broadcasted_iota(jnp.int32, (heads, rows), 0)
    pick[...] = (lane // head == row // share).astype(F32).astype(BF16)

    pltpu.make_async_copy(q_hbm, q_ref, qsem).wait()
    widen(0, 0)
    widen(1, 1)
    keys(0).wait()
    block((0, qbd0, s0))
    keys(KDEPTH).start()
    keys(1).wait()
    widen(2, 0)
    block((1, qbd1, s1), (0, s0, p0))
    pl.semaphore_wait(barrier, n - 1)

    def pair(late, first, j, carry):
        step(2 * j, 0, late, first)
        step(2 * j + 1, 1, late)
        return carry

    lax.fori_loop(1, 3, lambda j, c: pair(False, True, j, c), 0)
    lax.fori_loop(3, count // 2, lambda j, c: pair(True, False, j, c), 0)

    last = count - 1
    for copy in sends(last - 2):
        copy.start()
    values(last - 1).wait()
    block(None, (last, s1, p1), (last - 1, p0))
    for copy in sends(last - 1):
        copy.start()
    values(last).wait()
    block(None, None, (last, p1))
    for copy in sends(last):
        copy.start()

    def rest(i, carry):
        arrive(i)
        together(i)
        return carry

    lax.fori_loop(last - 2 - WAIT, count, rest, 0)


def solution(mesh):
    n = mesh.shape["sp"]

    def step(q, k, v):
        count, run, groups, head = k.shape
        heads = q.shape[1]
        rows = groups * head
        k, v = (a.transpose(0, 2, 3, 1).reshape(count, rows, run) for a in (k, v))

        def body(*refs):
            kernel(n, groups, heads // groups, *refs)

        return pl.pallas_call(
            body,
            out_shape=jax.ShapeDtypeStruct((count, heads, head), BF16),
            in_specs=[pl.BlockSpec(memory_space=pl.ANY)] * 3,
            out_specs=pl.BlockSpec(memory_space=pltpu.VMEM),
            scratch_shapes=[
                pltpu.VMEM((count, heads, head), BF16),
                pltpu.VMEM((KDEPTH, rows, run + PAD), BF16),
                pltpu.VMEM((VDEPTH, rows, run + PAD), BF16),
                pltpu.VMEM((head, rows), BF16),
                pltpu.VMEM((heads, rows), BF16),
                pltpu.VMEM((heads, rows), BF16),
                pltpu.VMEM((heads, rows), BF16),
                pltpu.VMEM((heads, run), F32),
                pltpu.VMEM((heads, run), F32),
                pltpu.VMEM((heads, run), BF16),
                pltpu.VMEM((heads, run), BF16),
                pltpu.VMEM((n, RING, head, 128), BF16),
                pltpu.VMEM((n, RING, 2, 128), F32),
                pltpu.VMEM((n - 1, head // 2 + 2, 128), F32),
                pltpu.SemaphoreType.DMA,
                pltpu.SemaphoreType.DMA((KDEPTH,)),
                pltpu.SemaphoreType.DMA((VDEPTH,)),
                pltpu.SemaphoreType.DMA((RING,)),
                pltpu.SemaphoreType.DMA((RING,)),
            ],
            compiler_params=pltpu.CompilerParams(
                collective_id=0, has_side_effects=True, vmem_limit_bytes=54125 * 1024
            ),
        )(q, k, v)

    return jax.shard_map(
        step,
        mesh=mesh,
        in_specs=(P("dp", None, None), P("dp", "sp", None, None), P("dp", "sp", None, None)),
        out_specs=P("dp", None, None),
        check_vma=False,
    )
```

```python
import math

import jax
import jax.numpy as jnp
from jax import lax
from jax.experimental import pallas as pl
from jax.experimental.pallas import tpu as pltpu
from jax.sharding import PartitionSpec as P

KDEPTH, VDEPTH = 4, 4
WAIT = 3
RING = 12
PAD = 256
TILE = 256
AHEAD = 4 * TILE
F32, BF16 = jnp.float32, jnp.bfloat16
MESH = pl.DeviceIdType.MESH


def kernel(n, groups, share, q_hbm, k_hbm, v_hbm, out_ref, q_ref, kbuf, vbuf, spread, pick, qbd0, qbd1, s0, s1, p0, p1, parts, stats, tally, qsem, ksem, vsem, send_sem, recv_sem):
    count, heads, head = q_ref.shape
    rows, run = k_hbm.shape[1], k_hbm.shape[2]
    half = rows // 2
    factor = head**-0.5 * math.log2(math.e)
    me = lax.axis_index("sp")
    peers = [lax.rem(me + d, n) for d in range(1, n)]
    qbd, score, prob = (qbd0, qbd1), (s0, s1), (p0, p1)

    def keys(i):
        slot = lax.rem(i, KDEPTH)
        return pltpu.make_async_copy(k_hbm.at[i], kbuf.at[slot, :, :run], ksem.at[slot])

    def values(i):
        slot = lax.rem(i, VDEPTH)
        return pltpu.make_async_copy(v_hbm.at[i], vbuf.at[slot, :, :run], vsem.at[slot])

    def sends(i):
        slot = lax.rem(i, RING)
        return [
            pltpu.make_async_remote_copy(
                src_ref=ref.at[me, slot],
                dst_ref=ref.at[me, slot],
                send_sem=send_sem.at[slot],
                recv_sem=recv_sem.at[slot],
                device_id={"sp": peer},
                device_id_type=MESH,
            )
            for peer in peers
            for ref in (parts, stats)
        ]

    def arrive(i):
        for sem in (send_sem, recv_sem):
            pltpu.make_async_copy(tally, tally, sem.at[lax.rem(i, RING)]).wait()

    def widen(i, side):
        wide = jnp.dot(q_ref[i], spread[...], preferred_element_type=F32).astype(BF16)
        qbd[side][...] = wide * pick[...]

    def together(i):
        slot = lax.rem(i, RING)
        high = [stats[d, slot, 0:1, :heads] for d in range(n)]
        total = [stats[d, slot, 1:2, :heads] for d in range(n)]
        top = high[0]
        for h in high[1:]:
            top = jnp.maximum(top, h)
        scale = [jnp.exp2((h - top) * factor) for h in high]
        whole = total[0] * scale[0]
        for t, c in zip(total[1:], scale[1:]):
            whole += t * c
        acc = parts[0, slot, :, :heads].astype(F32) * scale[0]
        for d in range(1, n):
            acc += parts[d, slot, :, :heads].astype(F32) * scale[d]
        out_ref[i] = (acc / whole).T.astype(BF16)

    def block(scores=None, soften=None, add=None, ahead=0):
        if soften is not None:
            s_in, p_out = soften[1:]
            high = s_in[:, :128]
            for c in range(128, run, 128):
                high = jnp.maximum(high, s_in[:, c : c + 128])
            high = jnp.max(high, -1, keepdims=True)
            total = jnp.zeros((heads, 128), F32)
        seen = {}

        def mark(t):
            tile = slice(t, t + TILE)
            i, q_in, s_out = scores
            s_out[:, tile] = jnp.dot(q_in[...], kbuf[lax.rem(i, KDEPTH), :, tile], preferred_element_type=F32)

        for t in range(0, ahead, TILE):
            mark(t)
        if ahead:
            values(add[0]).wait()
        for t in range(0, run, TILE):
            tile = slice(t, t + TILE)
            if add is not None:
                for a in range(2):
                    v = vbuf[lax.rem(add[0], VDEPTH), a * half : (a + 1) * half, tile]
                    d = lax.dot_general(v, add[1][:, tile], (((1,), (1,)), ((), ())), preferred_element_type=F32)
                    seen[a] = seen[a] + d if a in seen else d
            if scores is not None and t >= ahead:
                mark(t)
            if soften is not None:
                p = jnp.exp2((s_in[:, tile] - high) * factor)
                p_out[:, tile] = p.astype(BF16)
                for c in range(0, TILE, 128):
                    total += p[:, c : c + 128]
        if soften is not None:
            total = jnp.sum(total, -1, keepdims=True)
            spot = lax.broadcasted_iota(jnp.int32, (heads, 128), 1)
            both = jnp.where(spot == 0, high, total)
            stats[me, lax.rem(soften[0], RING), :, :heads] = both.T[:2]
        if add is not None:
            column = lax.broadcasted_iota(jnp.int32, (head, heads), 1)
            part = jnp.zeros((head, heads), F32)
            for a in range(2):
                for b in range(groups // 2):
                    g = a * groups // 2 + b
                    here = (column >= g * share) & (column < (g + 1) * share)
                    part = jnp.where(here, seen[a][b * head : (b + 1) * head], part)
            parts[me, lax.rem(add[0], RING), :, :heads] = part.astype(BF16)

    def start(i):
        @pl.when(i - 1 + KDEPTH < count)
        def _():
            keys(i - 1 + KDEPTH).start()

        @pl.when(i - 3 + VDEPTH < count)
        def _():
            values(i - 3 + VDEPTH).start()

    def step(i, a, late, first=False):
        if first:

            @pl.when(i >= 3)
            def _():
                start(i)
                for copy in sends(i - 3):
                    copy.start()

            @pl.when(i < 3)
            def _():
                keys(i - 1 + KDEPTH).start()
        else:
            start(i)
            for copy in sends(i - 3):
                copy.start()
        if late:
            arrive(i - 3 - WAIT)
        keys(i).wait()
        values(i - 2).wait()
        if late:
            together(i - 3 - WAIT)
        widen(jnp.minimum(i + 1, count - 1), 1 - a)
        block((i, qbd[a], score[a]), (i - 1, score[1 - a], prob[1 - a]), (i - 2, prob[a]))

    keys(0).start()
    pltpu.make_async_copy(q_hbm, q_ref, qsem).start()
    for i in range(1, VDEPTH + 2):
        if i < KDEPTH:
            keys(i).start()
        if i >= 2:
            values(i - 2).start()

    barrier = pltpu.get_barrier_semaphore()
    for peer in peers:
        pl.semaphore_signal(barrier, inc=1, device_id={"sp": peer}, device_id_type=MESH)

    lane = lax.broadcasted_iota(jnp.int32, (head, rows), 1)
    row = lax.broadcasted_iota(jnp.int32, (head, rows), 0)
    spread[...] = (lax.rem(lane, head) == row).astype(F32).astype(BF16)
    lane = lax.broadcasted_iota(jnp.int32, (heads, rows), 1)
    row = lax.broadcasted_iota(jnp.int32, (heads, rows), 0)
    pick[...] = (lane // head == row // share).astype(F32).astype(BF16)

    pltpu.make_async_copy(q_hbm, q_ref, qsem).wait()
    widen(0, 0)
    widen(1, 1)
    keys(0).wait()
    block((0, qbd0, s0))
    keys(KDEPTH).start()
    keys(1).wait()
    widen(2, 0)
    block((1, qbd1, s1), (0, s0, p0))
    pl.semaphore_wait(barrier, n - 1)

    def pair(late, first, j, carry):
        step(2 * j, 0, late, first)
        step(2 * j + 1, 1, late)
        return carry

    lax.fori_loop(1, 3, lambda j, c: pair(False, True, j, c), 0)
    lax.fori_loop(3, count // 2 - 1, lambda j, c: pair(True, False, j, c), 0)

    last = count - 1
    values(last).start()
    for i, a in ((last - 1, 0), (last, 1)):
        for copy in sends(i - 3):
            copy.start()
        keys(i).wait()
        if i < last:
            widen(last, 1)
        block((i, qbd[a], score[a]), (i - 1, score[1 - a], prob[1 - a]), (i - 2, prob[a]), AHEAD)
    for copy in sends(last - 2):
        copy.start()
    values(last - 1).wait()
    block(None, (last, s1, p1), (last - 1, p0))
    for copy in sends(last - 1):
        copy.start()
    values(last).wait()
    block(None, None, (last, p1))
    for copy in sends(last):
        copy.start()

    def rest(i, carry):
        arrive(i)
        together(i)
        return carry

    lax.fori_loop(last - 4 - WAIT, count, rest, 0)


def solution(mesh):
    n = mesh.shape["sp"]

    def step(q, k, v):
        count, run, groups, head = k.shape
        heads = q.shape[1]
        rows = groups * head
        k, v = (a.transpose(0, 2, 3, 1).reshape(count, rows, run) for a in (k, v))

        def body(*refs):
            kernel(n, groups, heads // groups, *refs)

        return pl.pallas_call(
            body,
            out_shape=jax.ShapeDtypeStruct((count, heads, head), BF16),
            in_specs=[pl.BlockSpec(memory_space=pl.ANY)] * 3,
            out_specs=pl.BlockSpec(memory_space=pltpu.VMEM),
            scratch_shapes=[
                pltpu.VMEM((count, heads, head), BF16),
                pltpu.VMEM((KDEPTH, rows, run + PAD), BF16),
                pltpu.VMEM((VDEPTH, rows, run + PAD), BF16),
                pltpu.VMEM((head, rows), BF16),
                pltpu.VMEM((heads, rows), BF16),
                pltpu.VMEM((heads, rows), BF16),
                pltpu.VMEM((heads, rows), BF16),
                pltpu.VMEM((heads, run), F32),
                pltpu.VMEM((heads, run), F32),
                pltpu.VMEM((heads, run), BF16),
                pltpu.VMEM((heads, run), BF16),
                pltpu.VMEM((n, RING, head, 128), BF16),
                pltpu.VMEM((n, RING, 2, 128), F32),
                pltpu.VMEM((n - 1, head // 2 + 2, 128), F32),
                pltpu.SemaphoreType.DMA,
                pltpu.SemaphoreType.DMA((KDEPTH,)),
                pltpu.SemaphoreType.DMA((VDEPTH,)),
                pltpu.SemaphoreType.DMA((RING,)),
                pltpu.SemaphoreType.DMA((RING,)),
            ],
            compiler_params=pltpu.CompilerParams(
                collective_id=0, has_side_effects=True, vmem_limit_bytes=54125 * 1024
            ),
        )(q, k, v)

    return jax.shard_map(
        step,
        mesh=mesh,
        in_specs=(P("dp", None, None), P("dp", "sp", None, None), P("dp", "sp", None, None)),
        out_specs=P("dp", None, None),
        check_vma=False,
    )
```

```python
import math

import jax
import jax.numpy as jnp
from jax import lax
from jax.experimental import pallas as pl
from jax.experimental.pallas import tpu as pltpu
from jax.sharding import PartitionSpec as P

KDEPTH, VDEPTH = 4, 4
WAIT = 3
RING = 12
PAD = 256
TILE = 256
AHEAD = 4 * TILE
F32, BF16 = jnp.float32, jnp.bfloat16
MESH = pl.DeviceIdType.MESH


def kernel(n, groups, share, q_hbm, k_hbm, v_hbm, out_ref, q_ref, kbuf, vbuf, spread, pick, qbd0, qbd1, s0, s1, p0, p1, parts, stats, tally, qsem, ksem, vsem, send_sem, recv_sem):
    count, heads, head = q_ref.shape
    rows, run = k_hbm.shape[1], k_hbm.shape[2]
    half = rows // 2
    factor = head**-0.5 * math.log2(math.e)
    me = lax.axis_index("sp")
    peers = [lax.rem(me + d, n) for d in range(1, n)]
    qbd, score, prob = (qbd0, qbd1), (s0, s1), (p0, p1)

    def keys(i):
        slot = lax.rem(i, KDEPTH)
        return pltpu.make_async_copy(k_hbm.at[i], kbuf.at[slot, :, :run], ksem.at[slot])

    def values(i):
        slot = lax.rem(i, VDEPTH)
        return pltpu.make_async_copy(v_hbm.at[i], vbuf.at[slot, :, :run], vsem.at[slot])

    def sends(i):
        slot = lax.rem(i, RING)
        return [
            pltpu.make_async_remote_copy(
                src_ref=ref.at[me, slot],
                dst_ref=ref.at[me, slot],
                send_sem=send_sem.at[slot],
                recv_sem=recv_sem.at[slot],
                device_id={"sp": peer},
                device_id_type=MESH,
            )
            for peer in peers
            for ref in (parts, stats)
        ]

    def arrive(i):
        for sem in (send_sem, recv_sem):
            pltpu.make_async_copy(tally, tally, sem.at[lax.rem(i, RING)]).wait()

    def widen(i, side):
        wide = jnp.dot(q_ref[i], spread[...], preferred_element_type=F32).astype(BF16)
        qbd[side][...] = wide * pick[...]

    def together(i):
        slot = lax.rem(i, RING)
        high = [stats[d, slot, 0:1, :heads] for d in range(n)]
        total = [stats[d, slot, 1:2, :heads] for d in range(n)]
        top = high[0]
        for h in high[1:]:
            top = jnp.maximum(top, h)
        scale = [jnp.exp2((h - top) * factor) for h in high]
        whole = total[0] * scale[0]
        for t, c in zip(total[1:], scale[1:]):
            whole += t * c
        acc = parts[0, slot, :, :heads].astype(F32) * scale[0]
        for d in range(1, n):
            acc += parts[d, slot, :, :heads].astype(F32) * scale[d]
        out_ref[i] = (acc / whole).T.astype(BF16)

    def block(scores=None, soften=None, add=None, ahead=0):
        if soften is not None:
            s_in, p_out = soften[1:]
            high = s_in[:, :128]
            for c in range(128, run, 128):
                high = jnp.maximum(high, s_in[:, c : c + 128])
            high = jnp.max(high, -1, keepdims=True)
            total = jnp.zeros((heads, 128), F32)
        seen = {}

        def mark(t):
            tile = slice(t, t + TILE)
            i, q_in, s_out = scores
            s_out[:, tile] = jnp.dot(q_in[...], kbuf[lax.rem(i, KDEPTH), :, tile], preferred_element_type=F32)

        for t in range(0, ahead, TILE):
            mark(t)
        if ahead:
            values(add[0]).wait()
        for t in range(0, run, TILE):
            tile = slice(t, t + TILE)
            if add is not None:
                for a in range(2):
                    v = vbuf[lax.rem(add[0], VDEPTH), a * half : (a + 1) * half, tile]
                    d = lax.dot_general(v, add[1][:, tile], (((1,), (1,)), ((), ())), preferred_element_type=F32)
                    seen[a] = seen[a] + d if a in seen else d
            if scores is not None and t >= ahead:
                mark(t)
            if soften is not None:
                p = jnp.exp2((s_in[:, tile] - high) * factor)
                p_out[:, tile] = p.astype(BF16)
                for c in range(0, TILE, 128):
                    total += p[:, c : c + 128]
        if soften is not None:
            total = jnp.sum(total, -1, keepdims=True)
            spot = lax.broadcasted_iota(jnp.int32, (heads, 128), 1)
            both = jnp.where(spot == 0, high, total)
            stats[me, lax.rem(soften[0], RING), :, :heads] = both.T[:2]
        if add is not None:
            column = lax.broadcasted_iota(jnp.int32, (head, heads), 1)
            part = jnp.zeros((head, heads), F32)
            for a in range(2):
                for b in range(groups // 2):
                    g = a * groups // 2 + b
                    here = (column >= g * share) & (column < (g + 1) * share)
                    part = jnp.where(here, seen[a][b * head : (b + 1) * head], part)
            parts[me, lax.rem(add[0], RING), :, :heads] = part.astype(BF16)

    def start(i):
        @pl.when(i - 1 + KDEPTH < count)
        def _():
            keys(i - 1 + KDEPTH).start()

        @pl.when(i - 3 + VDEPTH < count)
        def _():
            values(i - 3 + VDEPTH).start()

    def step(i, a, late, first=False):
        if first:

            @pl.when(i >= 3)
            def _():
                start(i)
                for copy in sends(i - 3):
                    copy.start()

            @pl.when(i < 3)
            def _():
                keys(i - 1 + KDEPTH).start()
        else:
            start(i)
            for copy in sends(i - 3):
                copy.start()
        if late:
            arrive(i - 3 - WAIT)
        keys(i).wait()
        values(i - 2).wait()
        if late:
            together(i - 3 - WAIT)
        widen(jnp.minimum(i + 1, count - 1), 1 - a)
        block((i, qbd[a], score[a]), (i - 1, score[1 - a], prob[1 - a]), (i - 2, prob[a]))

    keys(0).start()
    pltpu.make_async_copy(q_hbm, q_ref, qsem).start()
    barrier = pltpu.get_barrier_semaphore()
    for peer in peers:
        pl.semaphore_signal(barrier, inc=1, device_id={"sp": peer}, device_id_type=MESH)
    for i in range(1, VDEPTH + 2):
        if i < KDEPTH:
            keys(i).start()
        if i >= 2:
            values(i - 2).start()

    lane = lax.broadcasted_iota(jnp.int32, (head, rows), 1)
    row = lax.broadcasted_iota(jnp.int32, (head, rows), 0)
    spread[...] = (lax.rem(lane, head) == row).astype(F32).astype(BF16)
    lane = lax.broadcasted_iota(jnp.int32, (heads, rows), 1)
    row = lax.broadcasted_iota(jnp.int32, (heads, rows), 0)
    pick[...] = (lane // head == row // share).astype(F32).astype(BF16)

    pltpu.make_async_copy(q_hbm, q_ref, qsem).wait()
    widen(0, 0)
    widen(1, 1)
    keys(0).wait()
    block((0, qbd0, s0))
    keys(KDEPTH).start()
    keys(1).wait()
    widen(2, 0)
    block((1, qbd1, s1), (0, s0, p0))
    pl.semaphore_wait(barrier, n - 1)

    def pair(late, first, j, carry):
        step(2 * j, 0, late, first)
        step(2 * j + 1, 1, late)
        return carry

    lax.fori_loop(1, 3, lambda j, c: pair(False, True, j, c), 0)
    lax.fori_loop(3, count // 2 - 1, lambda j, c: pair(True, False, j, c), 0)

    last = count - 1
    values(last).start()
    for i, a in ((last - 1, 0), (last, 1)):
        for copy in sends(i - 3):
            copy.start()
        keys(i).wait()
        if i < last:
            widen(last, 1)
        block((i, qbd[a], score[a]), (i - 1, score[1 - a], prob[1 - a]), (i - 2, prob[a]), AHEAD)
    for copy in sends(last - 2):
        copy.start()
    values(last - 1).wait()
    block(None, (last, s1, p1), (last - 1, p0))
    for copy in sends(last - 1):
        copy.start()
    values(last).wait()
    block(None, None, (last, p1))
    for copy in sends(last):
        copy.start()

    def rest(i, carry):
        arrive(i)
        together(i)
        return carry

    lax.fori_loop(last - 4 - WAIT, count, rest, 0)


def solution(mesh):
    n = mesh.shape["sp"]

    def step(q, k, v):
        count, run, groups, head = k.shape
        heads = q.shape[1]
        rows = groups * head
        k, v = (a.transpose(0, 2, 3, 1).reshape(count, rows, run) for a in (k, v))

        def body(*refs):
            kernel(n, groups, heads // groups, *refs)

        return pl.pallas_call(
            body,
            out_shape=jax.ShapeDtypeStruct((count, heads, head), BF16),
            in_specs=[pl.BlockSpec(memory_space=pl.ANY)] * 3,
            out_specs=pl.BlockSpec(memory_space=pltpu.VMEM),
            scratch_shapes=[
                pltpu.VMEM((count, heads, head), BF16),
                pltpu.VMEM((KDEPTH, rows, run + PAD), BF16),
                pltpu.VMEM((VDEPTH, rows, run + PAD), BF16),
                pltpu.VMEM((head, rows), BF16),
                pltpu.VMEM((heads, rows), BF16),
                pltpu.VMEM((heads, rows), BF16),
                pltpu.VMEM((heads, rows), BF16),
                pltpu.VMEM((heads, run), F32),
                pltpu.VMEM((heads, run), F32),
                pltpu.VMEM((heads, run), BF16),
                pltpu.VMEM((heads, run), BF16),
                pltpu.VMEM((n, RING, head, 128), BF16),
                pltpu.VMEM((n, RING, 2, 128), F32),
                pltpu.VMEM((n - 1, head // 2 + 2, 128), F32),
                pltpu.SemaphoreType.DMA,
                pltpu.SemaphoreType.DMA((KDEPTH,)),
                pltpu.SemaphoreType.DMA((VDEPTH,)),
                pltpu.SemaphoreType.DMA((RING,)),
                pltpu.SemaphoreType.DMA((RING,)),
            ],
            compiler_params=pltpu.CompilerParams(
                collective_id=0,
                has_side_effects=True,
                vmem_limit_bytes=54125 * 1024,
            ),
        )(q, k, v)

    return jax.shard_map(
        step,
        mesh=mesh,
        in_specs=(P("dp", None, None), P("dp", "sp", None, None), P("dp", "sp", None, None)),
        out_specs=P("dp", None, None),
        check_vma=False,
    )
```

```python
import math

import jax
import jax.numpy as jnp
from jax import lax
from jax.experimental import pallas as pl
from jax.experimental.pallas import tpu as pltpu
from jax.sharding import PartitionSpec as P

KDEPTH, VDEPTH = 4, 4
WAIT = 3
RING = 12
PAD = 256
TILE = 256
AHEAD = 4 * TILE
F32, BF16 = jnp.float32, jnp.bfloat16
MESH = pl.DeviceIdType.MESH


def kernel(n, groups, share, q_hbm, k_hbm, v_hbm, out_ref, q_ref, kbuf, vbuf, spread, pick, qbd0, qbd1, s0, s1, p0, p1, parts, stats, tally, tally_parts, tally_stats, qsem, ksem, vsem, send_sem, recv_sem):
    count, heads, head = q_ref.shape
    rows, run = k_hbm.shape[1], k_hbm.shape[2]
    half = rows // 2
    factor = head**-0.5 * math.log2(math.e)
    me = lax.axis_index("sp")
    peers = [lax.rem(me + d, n) for d in range(1, n)]
    qbd, score, prob = (qbd0, qbd1), (s0, s1), (p0, p1)

    def keys(i):
        slot = lax.rem(i, KDEPTH)
        return pltpu.make_async_copy(k_hbm.at[i], kbuf.at[slot, :, :run], ksem.at[slot])

    def values(i):
        slot = lax.rem(i, VDEPTH)
        return pltpu.make_async_copy(v_hbm.at[i], vbuf.at[slot, :, :run], vsem.at[slot])

    def sends(i, refs=(parts, stats), sem=None):
        slot = lax.rem(i, RING)
        sem = slot if sem is None else sem
        return [
            pltpu.make_async_remote_copy(
                src_ref=ref.at[me, slot],
                dst_ref=ref.at[me, slot],
                send_sem=send_sem.at[sem],
                recv_sem=recv_sem.at[sem],
                device_id={"sp": peer},
                device_id_type=MESH,
            )
            for peer in peers
            for ref in refs
        ]

    def arrive(i):
        for sem in (send_sem, recv_sem):
            pltpu.make_async_copy(tally, tally, sem.at[lax.rem(i, RING)]).wait()

    def widen(i, side):
        wide = jnp.dot(q_ref[i], spread[...], preferred_element_type=F32).astype(BF16)
        qbd[side][...] = wide * pick[...]

    def shares(i):
        slot = lax.rem(i, RING)
        high = [stats[d, slot, 0:1, :heads] for d in range(n)]
        total = [stats[d, slot, 1:2, :heads] for d in range(n)]
        top = high[0]
        for h in high[1:]:
            top = jnp.maximum(top, h)
        scale = [jnp.exp2((h - top) * factor) for h in high]
        whole = total[0] * scale[0]
        for t, c in zip(total[1:], scale[1:]):
            whole += t * c
        return [c / whole for c in scale]

    def gather(i, scale):
        slot = lax.rem(i, RING)
        acc = parts[0, slot, :, :heads].astype(F32) * scale[0]
        for d in range(1, n):
            acc += parts[d, slot, :, :heads].astype(F32) * scale[d]
        out_ref[i] = acc.T.astype(BF16)

    def together(i):
        gather(i, shares(i))

    def block(scores=None, soften=None, add=None, ahead=0):
        if soften is not None:
            s_in, p_out = soften[1:]
            high = s_in[:, :128]
            for c in range(128, run, 128):
                high = jnp.maximum(high, s_in[:, c : c + 128])
            high = jnp.max(high, -1, keepdims=True)
            total = jnp.zeros((heads, 128), F32)
        seen = {}

        def mark(t):
            tile = slice(t, t + TILE)
            i, q_in, s_out = scores
            s_out[:, tile] = jnp.dot(q_in[...], kbuf[lax.rem(i, KDEPTH), :, tile], preferred_element_type=F32)

        for t in range(0, ahead, TILE):
            mark(t)
        if ahead:
            values(add[0]).wait()
        for t in range(0, run, TILE):
            tile = slice(t, t + TILE)
            if add is not None:
                for a in range(2):
                    v = vbuf[lax.rem(add[0], VDEPTH), a * half : (a + 1) * half, tile]
                    d = lax.dot_general(v, add[1][:, tile], (((1,), (1,)), ((), ())), preferred_element_type=F32)
                    seen[a] = seen[a] + d if a in seen else d
            if scores is not None and t >= ahead:
                mark(t)
            if soften is not None:
                p = jnp.exp2((s_in[:, tile] - high) * factor)
                p_out[:, tile] = p.astype(BF16)
                for c in range(0, TILE, 128):
                    total += p[:, c : c + 128]
        if soften is not None:
            total = jnp.sum(total, -1, keepdims=True)
            spot = lax.broadcasted_iota(jnp.int32, (heads, 128), 1)
            both = jnp.where(spot == 0, high, total)
            stats[me, lax.rem(soften[0], RING), :, :heads] = both.T[:2]
        if add is not None:
            column = lax.broadcasted_iota(jnp.int32, (head, heads), 1)
            part = jnp.zeros((head, heads), F32)
            for a in range(2):
                for b in range(groups // 2):
                    g = a * groups // 2 + b
                    here = (column >= g * share) & (column < (g + 1) * share)
                    part = jnp.where(here, seen[a][b * head : (b + 1) * head], part)
            parts[me, lax.rem(add[0], RING), :, :heads] = part.astype(BF16)

    def start(i):
        @pl.when(i - 1 + KDEPTH < count)
        def _():
            keys(i - 1 + KDEPTH).start()

        @pl.when(i - 3 + VDEPTH < count)
        def _():
            values(i - 3 + VDEPTH).start()

    def step(i, a, late, first=False):
        if first:

            @pl.when(i >= 3)
            def _():
                start(i)
                for copy in sends(i - 3):
                    copy.start()

            @pl.when(i < 3)
            def _():
                keys(i - 1 + KDEPTH).start()
        else:
            start(i)
            for copy in sends(i - 3):
                copy.start()
        if late:
            arrive(i - 3 - WAIT)
        keys(i).wait()
        values(i - 2).wait()
        if late:
            together(i - 3 - WAIT)
        widen(jnp.minimum(i + 1, count - 1), 1 - a)
        block((i, qbd[a], score[a]), (i - 1, score[1 - a], prob[1 - a]), (i - 2, prob[a]))

    keys(0).start()
    pltpu.make_async_copy(q_hbm, q_ref, qsem).start()
    barrier = pltpu.get_barrier_semaphore()
    for peer in peers:
        pl.semaphore_signal(barrier, inc=1, device_id={"sp": peer}, device_id_type=MESH)
    for i in range(1, VDEPTH + 2):
        if i < KDEPTH:
            keys(i).start()
        if i >= 2:
            values(i - 2).start()

    lane = lax.broadcasted_iota(jnp.int32, (head, rows), 1)
    row = lax.broadcasted_iota(jnp.int32, (head, rows), 0)
    spread[...] = (lax.rem(lane, head) == row).astype(F32).astype(BF16)
    lane = lax.broadcasted_iota(jnp.int32, (heads, rows), 1)
    row = lax.broadcasted_iota(jnp.int32, (heads, rows), 0)
    pick[...] = (lane // head == row // share).astype(F32).astype(BF16)

    pltpu.make_async_copy(q_hbm, q_ref, qsem).wait()
    widen(0, 0)
    widen(1, 1)
    keys(0).wait()
    block((0, qbd0, s0))
    keys(KDEPTH).start()
    keys(1).wait()
    widen(2, 0)
    block((1, qbd1, s1), (0, s0, p0))
    pl.semaphore_wait(barrier, n - 1)

    def pair(late, first, j, carry):
        step(2 * j, 0, late, first)
        step(2 * j + 1, 1, late)
        return carry

    lax.fori_loop(1, 3, lambda j, c: pair(False, True, j, c), 0)
    lax.fori_loop(3, count // 2 - 1, lambda j, c: pair(True, False, j, c), 0)

    last = count - 1
    values(last).start()
    for i, a in ((last - 1, 0), (last, 1)):
        for copy in sends(i - 3):
            copy.start()
        keys(i).wait()
        if i < last:
            widen(last, 1)
        block((i, qbd[a], score[a]), (i - 1, score[1 - a], prob[1 - a]), (i - 2, prob[a]), AHEAD)
    for copy in sends(last - 2):
        copy.start()
    values(last - 1).wait()
    block(None, (last, s1, p1), (last - 1, p0))
    for copy in sends(last - 1) + sends(last, (stats,), RING):
        copy.start()
    values(last).wait()
    block(None, None, (last, p1))
    for copy in sends(last, (parts,)):
        copy.start()

    def rest(i, carry):
        arrive(i)
        together(i)
        return carry

    lax.fori_loop(last - 4 - WAIT, last, rest, 0)
    for sem in (send_sem, recv_sem):
        pltpu.make_async_copy(tally_stats, tally_stats, sem.at[RING]).wait()
    scale = shares(last)
    for sem in (send_sem, recv_sem):
        pltpu.make_async_copy(tally_parts, tally_parts, sem.at[lax.rem(last, RING)]).wait()
    gather(last, scale)


def solution(mesh):
    n = mesh.shape["sp"]

    def step(q, k, v):
        count, run, groups, head = k.shape
        heads = q.shape[1]
        rows = groups * head
        k, v = (a.transpose(0, 2, 3, 1).reshape(count, rows, run) for a in (k, v))

        def body(*refs):
            kernel(n, groups, heads // groups, *refs)

        return pl.pallas_call(
            body,
            out_shape=jax.ShapeDtypeStruct((count, heads, head), BF16),
            in_specs=[pl.BlockSpec(memory_space=pl.ANY)] * 3,
            out_specs=pl.BlockSpec(memory_space=pltpu.VMEM),
            scratch_shapes=[
                pltpu.VMEM((count, heads, head), BF16),
                pltpu.VMEM((KDEPTH, rows, run + PAD), BF16),
                pltpu.VMEM((VDEPTH, rows, run + PAD), BF16),
                pltpu.VMEM((head, rows), BF16),
                pltpu.VMEM((heads, rows), BF16),
                pltpu.VMEM((heads, rows), BF16),
                pltpu.VMEM((heads, rows), BF16),
                pltpu.VMEM((heads, run), F32),
                pltpu.VMEM((heads, run), F32),
                pltpu.VMEM((heads, run), BF16),
                pltpu.VMEM((heads, run), BF16),
                pltpu.VMEM((n, RING, head, 128), BF16),
                pltpu.VMEM((n, RING, 2, 128), F32),
                pltpu.VMEM((n - 1, head // 2 + 2, 128), F32),
                pltpu.VMEM((n - 1, head // 2, 128), F32),
                pltpu.VMEM((n - 1, 2, 128), F32),
                pltpu.SemaphoreType.DMA,
                pltpu.SemaphoreType.DMA((KDEPTH,)),
                pltpu.SemaphoreType.DMA((VDEPTH,)),
                pltpu.SemaphoreType.DMA((RING + 1,)),
                pltpu.SemaphoreType.DMA((RING + 1,)),
            ],
            compiler_params=pltpu.CompilerParams(
                collective_id=0,
                has_side_effects=True,
                vmem_limit_bytes=54125 * 1024,
            ),
        )(q, k, v)

    return jax.shard_map(
        step,
        mesh=mesh,
        in_specs=(P("dp", None, None), P("dp", "sp", None, None), P("dp", "sp", None, None)),
        out_specs=P("dp", None, None),
        check_vma=False,
    )
```

```python
import math

import jax
import jax.numpy as jnp
from jax import lax
from jax.experimental import pallas as pl
from jax.experimental.pallas import tpu as pltpu
from jax.sharding import PartitionSpec as P

KDEPTH, VDEPTH = 4, 4
WAIT = 3
RING = 12
PAD = 128
TILE = 256
AHEAD = 4 * TILE
F32, BF16 = jnp.float32, jnp.bfloat16
MESH = pl.DeviceIdType.MESH


def kernel(n, groups, share, q_hbm, k_hbm, v_hbm, out_ref, q_ref, kbuf, vbuf, spread, pick, qbd0, qbd1, s0, s1, p0, p1, parts, stats, tally, qsem, ksem, vsem, send_sem, recv_sem):
    count, heads, head = q_ref.shape
    rows, run = k_hbm.shape[1], k_hbm.shape[2]
    half = rows // 2
    factor = head**-0.5 * math.log2(math.e)
    me = lax.axis_index("sp")
    peers = [lax.rem(me + d, n) for d in range(1, n)]
    qbd, score, prob = (qbd0, qbd1), (s0, s1), (p0, p1)

    def keys(i):
        slot = lax.rem(i, KDEPTH)
        return pltpu.make_async_copy(k_hbm.at[i], kbuf.at[slot, :, :run], ksem.at[slot])

    def values(i):
        slot = lax.rem(i, VDEPTH)
        return pltpu.make_async_copy(v_hbm.at[i], vbuf.at[slot, :, :run], vsem.at[slot])

    def sends(i):
        slot = lax.rem(i, RING)
        return [
            pltpu.make_async_remote_copy(
                src_ref=ref.at[me, slot],
                dst_ref=ref.at[me, slot],
                send_sem=send_sem.at[slot],
                recv_sem=recv_sem.at[slot],
                device_id={"sp": peer},
                device_id_type=MESH,
            )
            for peer in peers
            for ref in (parts, stats)
        ]

    def arrive(i):
        for sem in (send_sem, recv_sem):
            pltpu.make_async_copy(tally, tally, sem.at[lax.rem(i, RING)]).wait()

    def widen(i, side):
        wide = jnp.dot(q_ref[i], spread[...], preferred_element_type=F32).astype(BF16)
        qbd[side][...] = wide * pick[...]

    def together(i):
        slot = lax.rem(i, RING)
        high = [stats[d, slot, 0:1, :heads] for d in range(n)]
        total = [stats[d, slot, 1:2, :heads] for d in range(n)]
        top = high[0]
        for h in high[1:]:
            top = jnp.maximum(top, h)
        scale = [jnp.exp2((h - top) * factor) for h in high]
        whole = total[0] * scale[0]
        for t, c in zip(total[1:], scale[1:]):
            whole += t * c
        acc = parts[0, slot, :, :heads].astype(F32) * scale[0]
        for d in range(1, n):
            acc += parts[d, slot, :, :heads].astype(F32) * scale[d]
        out_ref[i] = (acc / whole).T.astype(BF16)

    def block(scores=None, soften=None, add=None, ahead=0):
        if soften is not None:
            s_in, p_out = soften[1:]
            high = s_in[:, :128]
            for c in range(128, run, 128):
                high = jnp.maximum(high, s_in[:, c : c + 128])
            high = jnp.max(high, -1, keepdims=True)
            total = jnp.zeros((heads, 128), F32)
        seen = {}

        def mark(t):
            tile = slice(t, t + TILE)
            i, q_in, s_out = scores
            s_out[:, tile] = jnp.dot(q_in[...], kbuf[lax.rem(i, KDEPTH), :, tile], preferred_element_type=F32)

        for t in range(0, ahead, TILE):
            mark(t)
        if ahead:
            values(add[0]).wait()
        for t in range(0, run, TILE):
            tile = slice(t, t + TILE)
            if add is not None:
                for a in range(2):
                    v = vbuf[lax.rem(add[0], VDEPTH), a * half : (a + 1) * half, tile]
                    d = lax.dot_general(v, add[1][:, tile], (((1,), (1,)), ((), ())), preferred_element_type=F32)
                    seen[a] = seen[a] + d if a in seen else d
            if scores is not None and t >= ahead:
                mark(t)
            if soften is not None:
                p = jnp.exp2((s_in[:, tile] - high) * factor)
                p_out[:, tile] = p.astype(BF16)
                for c in range(0, TILE, 128):
                    total += p[:, c : c + 128]
        if soften is not None:
            total = jnp.sum(total, -1, keepdims=True)
            spot = lax.broadcasted_iota(jnp.int32, (heads, 128), 1)
            both = jnp.where(spot == 0, high, total)
            stats[me, lax.rem(soften[0], RING), :, :heads] = both.T[:2]
        if add is not None:
            column = lax.broadcasted_iota(jnp.int32, (head, heads), 1)
            part = jnp.zeros((head, heads), F32)
            for a in range(2):
                for b in range(groups // 2):
                    g = a * groups // 2 + b
                    here = (column >= g * share) & (column < (g + 1) * share)
                    part = jnp.where(here, seen[a][b * head : (b + 1) * head], part)
            parts[me, lax.rem(add[0], RING), :, :heads] = part.astype(BF16)

    def start(i):
        @pl.when(i - 1 + KDEPTH < count)
        def _():
            keys(i - 1 + KDEPTH).start()

        @pl.when(i - 3 + VDEPTH < count)
        def _():
            values(i - 3 + VDEPTH).start()

    def step(i, a, late, first=False):
        if first:

            @pl.when(i >= 3)
            def _():
                start(i)
                for copy in sends(i - 3):
                    copy.start()

            @pl.when(i < 3)
            def _():
                keys(i - 1 + KDEPTH).start()
        else:
            start(i)
            for copy in sends(i - 3):
                copy.start()
        if late:
            arrive(i - 3 - WAIT)
        keys(i).wait()
        values(i - 2).wait()
        if late:
            together(i - 3 - WAIT)
        widen(jnp.minimum(i + 1, count - 1), 1 - a)
        block((i, qbd[a], score[a]), (i - 1, score[1 - a], prob[1 - a]), (i - 2, prob[a]))

    keys(0).start()
    pltpu.make_async_copy(q_hbm, q_ref, qsem).start()
    barrier = pltpu.get_barrier_semaphore()
    for peer in peers:
        pl.semaphore_signal(barrier, inc=1, device_id={"sp": peer}, device_id_type=MESH)
    for i in range(1, VDEPTH + 2):
        if i < KDEPTH:
            keys(i).start()
        if i >= 2:
            values(i - 2).start()

    lane = lax.broadcasted_iota(jnp.int32, (head, rows), 1)
    row = lax.broadcasted_iota(jnp.int32, (head, rows), 0)
    spread[...] = (lax.rem(lane, head) == row).astype(F32).astype(BF16)
    lane = lax.broadcasted_iota(jnp.int32, (heads, rows), 1)
    row = lax.broadcasted_iota(jnp.int32, (heads, rows), 0)
    pick[...] = (lane // head == row // share).astype(F32).astype(BF16)

    pltpu.make_async_copy(q_hbm, q_ref, qsem).wait()
    widen(0, 0)
    widen(1, 1)
    keys(0).wait()
    block((0, qbd0, s0))
    keys(KDEPTH).start()
    keys(1).wait()
    widen(2, 0)
    block((1, qbd1, s1), (0, s0, p0))
    pl.semaphore_wait(barrier, n - 1)

    def pair(late, first, j, carry):
        step(2 * j, 0, late, first)
        step(2 * j + 1, 1, late)
        return carry

    lax.fori_loop(1, 3, lambda j, c: pair(False, True, j, c), 0)
    lax.fori_loop(3, count // 2 - 1, lambda j, c: pair(True, False, j, c), 0)

    last = count - 1
    values(last).start()
    for i, a in ((last - 1, 0), (last, 1)):
        for copy in sends(i - 3):
            copy.start()
        keys(i).wait()
        if i < last:
            widen(last, 1)
        block((i, qbd[a], score[a]), (i - 1, score[1 - a], prob[1 - a]), (i - 2, prob[a]), AHEAD)
    for copy in sends(last - 2):
        copy.start()
    values(last - 1).wait()
    block(None, (last, s1, p1), (last - 1, p0))
    for copy in sends(last - 1):
        copy.start()
    values(last).wait()
    block(None, None, (last, p1))
    for copy in sends(last):
        copy.start()

    def rest(i, carry):
        arrive(i)
        together(i)
        return carry

    lax.fori_loop(last - 4 - WAIT, count, rest, 0)


def solution(mesh):
    n = mesh.shape["sp"]

    def step(q, k, v):
        count, run, groups, head = k.shape
        heads = q.shape[1]
        rows = groups * head
        k, v = (a.transpose(0, 2, 3, 1).reshape(count, rows, run) for a in (k, v))

        def body(*refs):
            kernel(n, groups, heads // groups, *refs)

        return pl.pallas_call(
            body,
            out_shape=jax.ShapeDtypeStruct((count, heads, head), BF16),
            in_specs=[pl.BlockSpec(memory_space=pl.ANY)] * 3,
            out_specs=pl.BlockSpec(memory_space=pltpu.VMEM),
            scratch_shapes=[
                pltpu.VMEM((count, heads, head), BF16),
                pltpu.VMEM((KDEPTH, rows, run + PAD), BF16),
                pltpu.VMEM((VDEPTH, rows, run + PAD), BF16),
                pltpu.VMEM((head, rows), BF16),
                pltpu.VMEM((heads, rows), BF16),
                pltpu.VMEM((heads, rows), BF16),
                pltpu.VMEM((heads, rows), BF16),
                pltpu.VMEM((heads, run), F32),
                pltpu.VMEM((heads, run), F32),
                pltpu.VMEM((heads, run), BF16),
                pltpu.VMEM((heads, run), BF16),
                pltpu.VMEM((n, RING, head, 128), BF16),
                pltpu.VMEM((n, RING, 2, 128), F32),
                pltpu.VMEM((n - 1, head // 2 + 2, 128), F32),
                pltpu.SemaphoreType.DMA,
                pltpu.SemaphoreType.DMA((KDEPTH,)),
                pltpu.SemaphoreType.DMA((VDEPTH,)),
                pltpu.SemaphoreType.DMA((RING,)),
                pltpu.SemaphoreType.DMA((RING,)),
            ],
            compiler_params=pltpu.CompilerParams(
                collective_id=0,
                has_side_effects=True,
                vmem_limit_bytes=54125 * 1024,
            ),
        )(q, k, v)

    return jax.shard_map(
        step,
        mesh=mesh,
        in_specs=(P("dp", None, None), P("dp", "sp", None, None), P("dp", "sp", None, None)),
        out_specs=P("dp", None, None),
        check_vma=False,
    )
```
